16 devices in a mesh: sub: 2 (over z), data: 8 (over y, x, core).
Axes of the slice: x: 2, y: 2, z: 2, core: 2. Of those that a mesh axis runs over, the one named last changes fastest.
Arguments:
- x_act: bfloat16 [96, 196, 512], P(('data', 'sub'))
- y_tgt: bfloat16 [96, 196, 512], P(('data', 'sub'))
- w_in: float32 [8, 512, 2048], replicated
- w_out: float32 [8, 2048, 512], replicated
Outputs:
- output 1: float32 [8, 512, 2048], replicated
- output 2: float32 [8, 2048, 512], replicated
- output 3: float32 [], replicated
All inputs are finite; a program needn't handle non-finite values.
Results may differ from the reference program's by a relative error of at most 0.00157091.
Values are sent between devices in bfloat16 or wider.
A program may use at most 1 GiB of HBM per device.

```python
import jax
import jax.numpy as jnp
from jax import lax

MODEL_DIM = 512
MLP_DIM = 2048
SEQ_LEN = 196
LAYERS = 8
IMAGES_DEV = 6
SUB_SIZE = 2
DATA_SIZE = 8
RHO_SCALE = 0.1
STEP_SIZE = 1.0


def setup_inputs(seed: int = 0) -> dict:
    root_key = jax.random.key(seed)
    key_x, key_y, key_in, key_out, key_scale = jax.random.split(root_key, 5)
    batch_size = IMAGES_DEV * SUB_SIZE * DATA_SIZE
    act_shape = (batch_size, SEQ_LEN, MODEL_DIM)
    x_act = jax.random.normal(key_x, act_shape, jnp.float32)
    y_tgt = jax.random.normal(key_y, act_shape, jnp.float32)
    w_in = jax.random.normal(key_in, (LAYERS, MODEL_DIM, MLP_DIM), jnp.float32) * MODEL_DIM ** -0.5
    layer_scale = jax.random.uniform(key_scale, (LAYERS, 1, 1), jnp.float32, 0.5, 1.5)
    w_out = jax.random.normal(key_out, (LAYERS, MLP_DIM, MODEL_DIM), jnp.float32) * layer_scale * (MLP_DIM * LAYERS) ** -0.5
    return {"x_act": x_act.astype(jnp.bfloat16), "y_tgt": y_tgt.astype(jnp.bfloat16), "w_in": w_in, "w_out": w_out}


def gelu_exact(pre_act):
    return jax.nn.gelu(pre_act, approximate=False)


def local_grads(tok_in, tok_tgt, w_in_b, w_out_b):
    def fwd_layer(hid_in, layer_w):
        w_in_l, w_out_l = layer_w
        pre_act = jnp.dot(hid_in, w_in_l, preferred_element_type=jnp.float32).astype(jnp.bfloat16)
        gelu_out = gelu_exact(pre_act.astype(jnp.float32)).astype(jnp.bfloat16)
        branch = jnp.dot(gelu_out, w_out_l, preferred_element_type=jnp.float32)
        hid_next = (hid_in.astype(jnp.float32) + branch).astype(jnp.bfloat16)
        return hid_next, (hid_in, pre_act, gelu_out)
    final_hid, saved_acts = lax.scan(fwd_layer, tok_in, (w_in_b, w_out_b))
    res_diff = final_hid.astype(jnp.float32) - tok_tgt.astype(jnp.float32)
    elem_count = res_diff.size
    loss_val = 0.5 * jnp.sum(res_diff * res_diff) / elem_count
    back_err = (res_diff / elem_count).astype(jnp.bfloat16)

    def bwd_layer(err_in, layer_data):
        w_in_l, w_out_l, hid_in, pre_act, gelu_out = layer_data
        grad_out = jnp.dot(gelu_out.T, err_in, preferred_element_type=jnp.float32).astype(jnp.bfloat16)
        d_act = jnp.dot(err_in, w_out_l.T, preferred_element_type=jnp.float32).astype(jnp.bfloat16)
        gelu_vjp = jax.vjp(gelu_exact, pre_act.astype(jnp.float32))[1]
        d_pre = gelu_vjp(d_act.astype(jnp.float32))[0].astype(jnp.bfloat16)
        grad_in = jnp.dot(hid_in.T, d_pre, preferred_element_type=jnp.float32).astype(jnp.bfloat16)
        err_next = (err_in.astype(jnp.float32) + jnp.dot(d_pre, w_in_l.T, preferred_element_type=jnp.float32)).astype(jnp.bfloat16)
        return err_next, (grad_in, grad_out)
    hid_acts, pre_acts, gelu_outs = saved_acts
    back_res = lax.scan(bwd_layer, back_err, (w_in_b, w_out_b, hid_acts, pre_acts, gelu_outs), reverse=True)
    grad_in, grad_out = back_res[1]
    return loss_val, grad_in, grad_out


def reference(x_act, y_tgt, w_in, w_out):
    tok_rows = IMAGES_DEV * SEQ_LEN
    dev_count = SUB_SIZE * DATA_SIZE
    x_dev = x_act.reshape(DATA_SIZE, SUB_SIZE, tok_rows, MODEL_DIM)
    y_dev = y_tgt.reshape(DATA_SIZE, SUB_SIZE, tok_rows, MODEL_DIM)
    rho_val = RHO_SCALE * MODEL_DIM ** 0.5
    w_in_b = w_in.astype(jnp.bfloat16)
    w_out_b = w_out.astype(jnp.bfloat16)
    zero_in = jnp.zeros(w_in.shape, jnp.float32)
    zero_out = jnp.zeros(w_out.shape, jnp.float32)

    def group_step(carry_sums, group_data):
        x_grp, y_grp = group_data

        def first_dev(acc_sums, dev_data):
            grads = local_grads(dev_data[0], dev_data[1], w_in_b, w_out_b)
            return (acc_sums[0] + grads[1].astype(jnp.float32), acc_sums[1] + grads[2].astype(jnp.float32)), None
        first_res = lax.scan(first_dev, (zero_in, zero_out), (x_grp, y_grp))
        mean_in = first_res[0][0] / SUB_SIZE
        mean_out = first_res[0][1] / SUB_SIZE
        grad_norm = jnp.sqrt(jnp.sum(mean_in * mean_in) + jnp.sum(mean_out * mean_out))
        eps_scale = rho_val / grad_norm
        pert_in = (w_in + eps_scale * mean_in).astype(jnp.bfloat16)
        pert_out = (w_out + eps_scale * mean_out).astype(jnp.bfloat16)

        def second_dev(acc_sums, dev_data):
            loss_val, grad_in, grad_out = local_grads(dev_data[0], dev_data[1], pert_in, pert_out)
            return (acc_sums[0] + grad_in.astype(jnp.float32), acc_sums[1] + grad_out.astype(jnp.float32), acc_sums[2] + loss_val), None
        second_res = lax.scan(second_dev, carry_sums, (x_grp, y_grp))
        return second_res[0], None

    totals = lax.scan(group_step, (zero_in, zero_out, jnp.zeros((), jnp.float32)), (x_dev, y_dev))[0]
    w_in_new = w_in - STEP_SIZE * (totals[0] / dev_count)
    w_out_new = w_out - STEP_SIZE * (totals[1] / dev_count)
    return w_in_new, w_out_new, totals[2] / dev_count
```

```python
import jax
import jax.numpy as jnp
from jax import lax
from jax.experimental.layout import Layout, with_layout_constraint
from jax.sharding import PartitionSpec as P

RHO_SCALE = 0.1
STEP_SIZE = 1.0
AXES = ("sub", "data")
F32, BF16 = jnp.float32, jnp.bfloat16


def gelu(z):
    return 0.5 * z * (1.0 + lax.erf(z * (0.5 ** 0.5)))


def gelu_slope(z):
    return 0.5 * (1.0 + lax.erf(z * (0.5 ** 0.5))) + z * (jnp.exp(-0.5 * z * z) * 0.3989422804014327)


def forward(hidden, w_in_b, w_out_b):
    saved = []
    for l in range(len(w_in_b)):
        pre = jnp.dot(hidden, w_in_b[l], preferred_element_type=F32).astype(BF16)
        act = gelu(pre.astype(F32)).astype(BF16)
        branch = jnp.dot(act, w_out_b[l], preferred_element_type=F32)
        saved.append((hidden, pre, act))
        hidden = (hidden.astype(F32) + branch).astype(BF16)
    return hidden, saved


def loss_and_err(hidden, target):
    diff = hidden.astype(F32) - target.astype(F32)
    return 0.5 * jnp.sum(diff * diff) / diff.size, (diff / diff.size).astype(BF16)


def rows_major(g):
    return with_layout_constraint(g, Layout(major_to_minor=(0, 1)))


def backward_layer(err, weights, saved, last):
    hid, pre, act = saved
    g_out = lax.dot_general(act, err, (((0,), (0,)), ((), ())), preferred_element_type=F32).astype(BF16)
    d_act = lax.dot_general(err, weights[1], (((1,), (1,)), ((), ())), preferred_element_type=F32).astype(BF16)
    d_pre = (gelu_slope(pre.astype(F32)) * d_act.astype(F32)).astype(BF16)
    g_in = lax.dot_general(hid, d_pre, (((0,), (0,)), ((), ())), preferred_element_type=F32).astype(BF16)
    if not last:
        err = (err.astype(F32) + lax.dot_general(d_pre, weights[0], (((1,), (1,)), ((), ())), preferred_element_type=F32)).astype(BF16)
    return err, rows_major(g_in), rows_major(g_out)


def solution(mesh):
    sub_size = mesh.shape["sub"]
    data_size = mesh.shape["data"]
    n = sub_size * data_size

    def flip(bit):
        return [(i, i ^ bit) for i in range(n)]

    regroup = []
    for i in range(n):
        z, yx, c = i // data_size, (i % data_size) // 2, i % 2
        regroup.append((i, c * data_size + yx * 2 + z))

    def device_step(x_blk, y_blk, w_in, w_out):
        layers, dim, _ = w_in.shape
        me = lax.axis_index("sub") * data_size + lax.axis_index("data")
        tok_in = lax.ppermute(x_blk.reshape(-1, dim), AXES, regroup)
        tok_tgt = lax.ppermute(y_blk.reshape(-1, dim), AXES, regroup)

        w_in_b, w_out_b = w_in.astype(BF16), w_out.astype(BF16)

        hidden, saved = forward(tok_in, w_in_b, w_out_b)
        err = loss_and_err(hidden, tok_tgt)[1]
        pair = [None] * layers
        waiting = None
        for l in reversed(range(layers)):
            away = waiting and [lax.ppermute(g, AXES, flip(1)) for g in waiting]
            grads = backward_layer(err, (w_in_b[l], w_out_b[l]), saved[l], l == 0)
            (err, g_in, g_out), away = lax.optimization_barrier((grads, away))
            if l + 1 < layers:
                pair[l + 1] = list(zip(waiting, away))
            waiting = (g_in, g_out)
        pair[0] = [(g, lax.ppermute(g, AXES, flip(1))) for g in waiting]
        mean = [[(a.astype(F32) + b.astype(F32)) / sub_size for a, b in p] for p in pair]
        squares = [jnp.sum((m * m).reshape(-1, 8, m.shape[1]), axis=0) for p in mean for m in p]
        norm_sq = sum(jnp.sum(q) for q in lax.optimization_barrier(squares))
        scale = RHO_SCALE * dim ** 0.5 / jnp.sqrt(norm_sq)
        pert_in = [(w_in[l] + scale * mean[l][0]).astype(BF16) for l in range(layers)]
        pert_out = [(w_out[l] + scale * mean[l][1]).astype(BF16) for l in range(layers)]

        axis_of = {8: 0, 4: 1, 2: 2, 1: 3}
        orders = ((1, 2, 4, 8), (1, 8, 4, 2))

        def halve(part, bit):
            mine = (me // bit) % 2
            ax = axis_of[bit]
            away = lax.ppermute(lax.dynamic_slice_in_dim(part, 1 - mine, 1, ax), AXES, flip(bit))
            return part, away

        def add(part, away, bit):
            return lax.dynamic_slice_in_dim(part, (me // bit) % 2, 1, axis_of[bit]).astype(F32) + away.astype(F32)

        def blocks(g):
            return g.reshape((2, 2, 2, 2, g.shape[0] // n, g.shape[1]))

        hidden, saved = forward(tok_in, pert_in, pert_out)
        loss, err = loss_and_err(hidden, tok_tgt)
        sums = [[None] * 2 for _ in range(layers)]
        pieces = [{}, {}]
        pipe = {}
        loss_bits = [1, 2, 4, 8]

        def gather(low, high):
            news = []
            for k, w in enumerate((w_in, w_out)):
                rows = w.shape[1] // n
                own = lax.dynamic_slice(w, (low, me * rows, 0), (high - low, rows, w.shape[2]))
                news.append(own - STEP_SIZE * (jnp.stack([s[k] for s in sums[low:high]]) / n))
            if low == 0:
                news, pieces[:] = lax.optimization_barrier((news, list(pieces)))
            for k, new in enumerate(news):
                pieces[k][low] = lax.all_gather(new, AXES, axis=1, tiled=True)

        for l in reversed(range(-4, layers)):
            sent = {(m, k, stage): halve(part, orders[k][stage]) for (m, k, stage), part in pipe.items()}
            more = lax.ppermute(loss, AXES, flip(loss_bits.pop(0))) if loss_bits else None
            grads = backward_layer(err, (pert_in[l], pert_out[l]), saved[l], l == 0) if l >= 0 else None
            grads, sent, more = lax.optimization_barrier((grads, sent, more))
            if more is not None:
                loss += more
            if l >= 0:
                err, g_in, g_out = grads
            pipe = {}
            for (m, k, stage), (part, away) in sent.items():
                part = add(part, away, orders[k][stage])
                if stage == 3:
                    sums[m][k] = part.reshape(part.shape[-2:])
                else:
                    pipe[m, k, stage + 1] = part
            if l >= 0:
                pipe[l, 0, 0], pipe[l, 1, 0] = blocks(g_in), blocks(g_out)
            for low, high in ((5, 8), (0, 5)):
                if l == low - 4:
                    gather(low, high)

        outs = [jnp.concatenate([p[low] for low in sorted(p)]) for p in pieces]
        return outs[0], outs[1], loss / n

    batch_spec = P(("data", "sub"))
    return jax.shard_map(device_step, mesh=mesh, in_specs=(batch_spec, batch_spec, P(), P()), out_specs=(P(), P(), P()), check_vma=False)
```
